32 devices in a mesh: fsdp: 32 (over z, y, x, core).
Axes of the slice: x: 2, y: 2, z: 4, core: 2. Of those that a mesh axis runs over, the one named last changes fastest.
Arguments:
- resid_in: bfloat16 [96, 257, 1408], P('fsdp')
- grad_out: bfloat16 [96, 257, 1408], P('fsdp')
- ln1_gain: float32 [1408], P('fsdp')
- ln1_bias: float32 [1408], P('fsdp')
- qkv_weight: float32 [1408, 4224], P('fsdp')
- qkv_bias: float32 [4224], P('fsdp')
- out_weight: float32 [1408, 1408], P('fsdp')
- out_bias: float32 [1408], P('fsdp')
- ln2_gain: float32 [1408], P('fsdp')
- ln2_bias: float32 [1408], P('fsdp')
- fc_weight: float32 [1408, 6144], P('fsdp')
- fc_bias: float32 [6144], P('fsdp')
- proj_weight: float32 [6144, 1408], P('fsdp')
- proj_bias: float32 [1408], P('fsdp')
Outputs:
- output 1: bfloat16 [96, 257, 1408], P('fsdp')
- output 2: bfloat16 [96, 257, 1408], P('fsdp')
- output 3: float32 [1408], P('fsdp')
- output 4: float32 [1408], P('fsdp')
- output 5: float32 [1408, 4224], P('fsdp')
- output 6: float32 [4224], P('fsdp')
- output 7: float32 [1408, 1408], P('fsdp')
- output 8: float32 [1408], P('fsdp')
- output 9: float32 [1408], P('fsdp')
- output 10: float32 [1408], P('fsdp')
- output 11: float32 [1408, 6144], P('fsdp')
- output 12: float32 [6144], P('fsdp')
- output 13: float32 [6144, 1408], P('fsdp')
- output 14: float32 [1408], P('fsdp')
All inputs are finite; a program needn't handle non-finite values.
Results may differ from the reference program's by a relative error of at most 0.02.
Values are sent between devices in bfloat16 or wider.
A program may use at most 1 GiB of HBM per device.

```python
import jax
import jax.numpy as jnp
from jax import lax

WIDTH = 1408
FFN = 6144
HEADS = 16
PATCHES = 256
BATCH = 96

SEQ = PATCHES + 1
HEAD_DIM = WIDTH // HEADS
LN_EPS = 1e-5


def setup_inputs(seed: int = 0) -> dict:
    keys = jax.random.split(jax.random.key(seed), 14)

    def normal(key_index, shape, scale):
        return jax.random.normal(keys[key_index], shape, jnp.float32) * scale

    return {
        "resid_in": normal(0, (BATCH, SEQ, WIDTH), 1.0).astype(jnp.bfloat16),
        "grad_out": normal(1, (BATCH, SEQ, WIDTH), 1.0).astype(jnp.bfloat16),
        "ln1_gain": 1.0 + normal(2, (WIDTH,), 0.6),
        "ln1_bias": normal(3, (WIDTH,), 1.0),
        "qkv_weight": normal(4, (WIDTH, 3 * WIDTH), WIDTH ** -0.5),
        "qkv_bias": normal(5, (3 * WIDTH,), 1.0),
        "out_weight": normal(6, (WIDTH, WIDTH), WIDTH ** -0.5),
        "out_bias": normal(7, (WIDTH,), 1.0),
        "ln2_gain": 1.0 + normal(8, (WIDTH,), 0.6),
        "ln2_bias": normal(9, (WIDTH,), 1.0),
        "fc_weight": normal(10, (WIDTH, FFN), WIDTH ** -0.5),
        "fc_bias": normal(11, (FFN,), 1.0),
        "proj_weight": normal(12, (FFN, WIDTH), FFN ** -0.5),
        "proj_bias": normal(13, (WIDTH,), 1.0),
    }


def layer_norm(values, gain, bias):
    mean_val = jnp.mean(values, axis=-1, keepdims=True)
    centered = values - mean_val
    variance = jnp.mean(centered * centered, axis=-1, keepdims=True)
    return centered * lax.rsqrt(variance + LN_EPS) * gain + bias


def layer_forward(params, tokens):
    (ln1_gain, ln1_bias, qkv_weight, qkv_bias, out_weight, out_bias,
     ln2_gain, ln2_bias, fc_weight, fc_bias, proj_weight, proj_bias) = [param.astype(jnp.bfloat16) for param in params]
    resid = tokens.astype(jnp.float32)
    normed_one = layer_norm(resid, ln1_gain, ln1_bias).astype(jnp.bfloat16)
    qkv_vals = (jnp.dot(normed_one, qkv_weight, preferred_element_type=jnp.float32) + qkv_bias).astype(jnp.bfloat16)
    qkv_vals = qkv_vals.reshape(SEQ, 3, HEADS, HEAD_DIM).astype(jnp.float32)
    scores = jnp.einsum("qhd,khd->hqk", qkv_vals[:, 0], qkv_vals[:, 1]) * (HEAD_DIM ** -0.5)
    attn_probs = jax.nn.softmax(scores, axis=-1).astype(jnp.bfloat16).astype(jnp.float32)
    mixed = jnp.einsum("hqk,khd->qhd", attn_probs, qkv_vals[:, 2]).astype(jnp.bfloat16).reshape(SEQ, WIDTH)
    middle = (resid + jnp.dot(mixed, out_weight, preferred_element_type=jnp.float32) + out_bias).astype(jnp.bfloat16)
    middle_wide = middle.astype(jnp.float32)
    normed_two = layer_norm(middle_wide, ln2_gain, ln2_bias).astype(jnp.bfloat16)
    pre_act = jnp.dot(normed_two, fc_weight, preferred_element_type=jnp.float32) + fc_bias
    hidden = jax.nn.gelu(pre_act, approximate=False).astype(jnp.bfloat16)
    return (middle_wide + jnp.dot(hidden, proj_weight, preferred_element_type=jnp.float32) + proj_bias).astype(jnp.bfloat16)


def reference(resid_in, grad_out, ln1_gain, ln1_bias, qkv_weight, qkv_bias, out_weight, out_bias,
              ln2_gain, ln2_bias, fc_weight, fc_bias, proj_weight, proj_bias):
    params = (ln1_gain, ln1_bias, qkv_weight, qkv_bias, out_weight, out_bias,
              ln2_gain, ln2_bias, fc_weight, fc_bias, proj_weight, proj_bias)

    def per_image(grad_sum, pair):
        tokens, cotangent = pair
        image_out, pullback = jax.vjp(layer_forward, params, tokens)
        param_grads, token_grad = pullback(cotangent)
        grad_sum = jax.tree.map(lambda total, fresh: total + fresh, grad_sum, param_grads)
        return grad_sum, (image_out, token_grad)

    start_sum = jax.tree.map(jnp.zeros_like, params)
    grad_sum, (resid_out, grad_in) = lax.scan(per_image, start_sum, (resid_in, grad_out))
    (grad_ln1_gain, grad_ln1_bias, grad_qkv_weight, grad_qkv_bias, grad_out_weight, grad_out_bias,
     grad_ln2_gain, grad_ln2_bias, grad_fc_weight, grad_fc_bias, grad_proj_weight, grad_proj_bias) = grad_sum
    return (resid_out, grad_in, grad_ln1_gain, grad_ln1_bias, grad_qkv_weight, grad_qkv_bias,
            grad_out_weight, grad_out_bias, grad_ln2_gain, grad_ln2_bias, grad_fc_weight, grad_fc_bias,
            grad_proj_weight, grad_proj_bias)
```

```python
import math
import jax
import jax.numpy as jnp
from jax import lax
from jax.experimental import pallas as pl
from jax.experimental.pallas import tpu as pltpu
from jax.sharding import PartitionSpec as P


HEADS = 16
LN_EPS = 1e-5
DEVICES = 32
ROWS = 44
ROWS_PAD = 48
PADDED = DEVICES * ROWS_PAD
QKV = 4224
LANES = 256
SMALL_AT = (0, 1, 3, 5, 6, 7, 9, 11)
SMALL = (44, 44, 132, 44, 44, 44, 192, 44)


HEAD_DIM = 88
WIDTH = 1408


def dot_nn(left, right):
    return lax.dot_general(left, right, (((1,), (0,)), ((), ())), preferred_element_type=jnp.float32)


def dot_nt(left, right):
    return lax.dot_general(left, right, (((1,), (1,)), ((), ())), preferred_element_type=jnp.float32)


def transposed_probs(query, key):
    scores = dot_nt(key, query) * (HEAD_DIM ** -0.5)
    weights = jnp.exp(scores - jnp.max(scores, axis=0, keepdims=True))
    return weights * (1.0 / jnp.sum(weights, axis=0, keepdims=True))


def attention_fwd_kernel(qkv_ref, mixed_ref):
    for head in range(HEADS):
        query, key, value = (qkv_ref[0, :, pl.ds(part * WIDTH + head * HEAD_DIM, HEAD_DIM)] for part in range(3))
        probs = transposed_probs(query, key).astype(jnp.bfloat16)
        mixed = dot_nn(value.T, probs)
        mixed_ref[0, :, pl.ds(head * HEAD_DIM, HEAD_DIM)] = mixed.T.astype(jnp.bfloat16)


def attention_bwd_kernel(qkv_ref, grad_mixed_ref, grad_qkv_ref, bias_ref):
    for head in range(HEADS):
        query, key, value = (qkv_ref[0, :, pl.ds(part * WIDTH + head * HEAD_DIM, HEAD_DIM)] for part in range(3))
        grad_mixed = grad_mixed_ref[0, :, pl.ds(head * HEAD_DIM, HEAD_DIM)]
        probs = transposed_probs(query, key)
        grad_probs = dot_nt(value, grad_mixed)
        grad_value = dot_nn(probs.astype(jnp.bfloat16), grad_mixed)
        inner = jnp.sum(grad_probs * probs, axis=0, keepdims=True)
        grad_scores = (probs * (grad_probs - inner) * (HEAD_DIM ** -0.5)).astype(jnp.bfloat16)
        grad_key = dot_nn(grad_scores, query)
        grad_query = dot_nn(key.T, grad_scores).T
        for part, grad in enumerate((grad_query, grad_key, grad_value)):
            lanes = pl.ds(part * WIDTH + head * HEAD_DIM, HEAD_DIM)
            grad_qkv_ref[0, :, lanes] = grad.astype(jnp.bfloat16)
            bias_ref[0, :, lanes] = jnp.sum(grad, axis=0, keepdims=True)


def image_block(rows, columns):
    return pl.BlockSpec((1, rows, columns), lambda image: (image, 0, 0))


def attention_fwd(qkv):
    images, tokens, _ = qkv.shape
    return pl.pallas_call(
        attention_fwd_kernel, grid=(images,), name="attention_fwd",
        in_specs=[image_block(tokens, 3 * WIDTH)], out_specs=image_block(tokens, WIDTH),
        out_shape=jax.ShapeDtypeStruct((images, tokens, WIDTH), jnp.bfloat16),
        compiler_params=pltpu.CompilerParams(vmem_limit_bytes=40 << 20),
        cost_estimate=pl.CostEstimate(flops=6_000_000_000, bytes_accessed=9_000_000, transcendentals=3_200_000),
    )(qkv)


def attention_bwd(qkv, grad_mixed):
    images, tokens, _ = qkv.shape
    return pl.pallas_call(
        attention_bwd_kernel, grid=(images,), name="attention_bwd",
        in_specs=[image_block(tokens, 3 * WIDTH), image_block(tokens, WIDTH)],
        out_specs=[image_block(tokens, 3 * WIDTH), image_block(1, 3 * WIDTH)],
        out_shape=[jax.ShapeDtypeStruct((images, tokens, 3 * WIDTH), jnp.bfloat16),
                   jax.ShapeDtypeStruct((images, 1, 3 * WIDTH), jnp.float32)],
        compiler_params=pltpu.CompilerParams(vmem_limit_bytes=40 << 20),
        cost_estimate=pl.CostEstimate(flops=16_000_000_000, bytes_accessed=16_000_000, transcendentals=3_200_000),
    )(qkv, grad_mixed)


def layer_norm_fwd(values, gain, bias):
    mean_val = jnp.mean(values, axis=-1, keepdims=True)
    centered = values - mean_val
    inv_std = lax.rsqrt(jnp.mean(centered * centered, axis=-1, keepdims=True) + LN_EPS)
    x_hat = centered * inv_std
    return x_hat * gain + bias, x_hat, inv_std


def layer_norm_bwd(grad_norm, x_hat, inv_std, gain):
    grad_hat = grad_norm * gain
    grad_vals = inv_std * (grad_hat - jnp.mean(grad_hat, axis=-1, keepdims=True)
                           - x_hat * jnp.mean(grad_hat * x_hat, axis=-1, keepdims=True))
    return grad_vals, jnp.sum(grad_norm * x_hat, axis=(0, 1)), jnp.sum(grad_norm, axis=(0, 1))


def forward_local(full, tokens):
    (ln1_gain, ln1_bias, qkv_weight, qkv_bias, out_weight, out_bias,
     ln2_gain, ln2_bias, fc_weight, fc_bias, proj_weight, proj_bias) = full
    resid = tokens.astype(jnp.float32)
    normed, hat_one, inv_one = layer_norm_fwd(resid, ln1_gain, ln1_bias)
    normed_one = normed.astype(jnp.bfloat16)
    qkv_vals = (jnp.einsum("bsw,wk->bsk", normed_one, qkv_weight, preferred_element_type=jnp.float32) + qkv_bias).astype(jnp.bfloat16)
    mixed = attention_fwd(qkv_vals)
    middle = (resid + jnp.einsum("bsw,wv->bsv", mixed, out_weight, preferred_element_type=jnp.float32) + out_bias).astype(jnp.bfloat16)
    middle_wide = middle.astype(jnp.float32)
    normed, hat_two, inv_two = layer_norm_fwd(middle_wide, ln2_gain, ln2_bias)
    normed_two = normed.astype(jnp.bfloat16)
    pre_act = jnp.einsum("bsw,wf->bsf", normed_two, fc_weight, preferred_element_type=jnp.float32) + fc_bias
    hidden = jax.nn.gelu(pre_act, approximate=False).astype(jnp.bfloat16)
    resid_out = (middle_wide + jnp.einsum("bsf,fw->bsw", hidden, proj_weight, preferred_element_type=jnp.float32) + proj_bias).astype(jnp.bfloat16)
    saved = (hat_one, inv_one, normed_one, qkv_vals, mixed, hat_two, inv_two, normed_two, pre_act, hidden)
    return resid_out, saved


def pad_rows(values):
    width = values.shape[-1]
    source = lax.broadcasted_iota(jnp.int32, (width, PADDED), 0)
    target = lax.broadcasted_iota(jnp.int32, (width, PADDED), 1)
    spread = (source // ROWS * ROWS_PAD + source % ROWS == target).astype(jnp.bfloat16)
    return jnp.einsum("bsw,wp->bsp", values, spread, preferred_element_type=jnp.float32).astype(jnp.bfloat16)


def backward_local(weights, saved, grad_out):
    (ln1_gain, qkv_weight, out_weight, ln2_gain, fc_weight, proj_weight) = weights
    (hat_one, inv_one, normed_one, qkv_vals, mixed, hat_two, inv_two, normed_two, pre_act, hidden) = saved
    grad_wide = grad_out.astype(jnp.float32)
    d_proj_weight = jnp.einsum("bsf,bsw->fw", hidden, grad_out, preferred_element_type=jnp.float32)
    d_proj_weight, grad_out = lax.optimization_barrier((d_proj_weight, grad_out))
    d_proj_bias = jnp.sum(grad_wide, axis=(0, 1))
    grad_hidden = jnp.einsum("bsw,fw->bsf", grad_out, proj_weight, preferred_element_type=jnp.float32)
    gauss_cdf = 0.5 * (1.0 + lax.erf(pre_act * (0.5 ** 0.5)))
    gauss_pdf = jnp.exp(-0.5 * pre_act * pre_act) * ((2.0 * math.pi) ** -0.5)
    grad_pre = grad_hidden * (gauss_cdf + pre_act * gauss_pdf)
    grad_pre_low = grad_pre.astype(jnp.bfloat16)
    d_fc_weight = jnp.einsum("bsw,bsf->wf", pad_rows(normed_two), grad_pre_low, preferred_element_type=jnp.float32)
    d_fc_weight, grad_pre_low = lax.optimization_barrier((d_fc_weight, grad_pre_low))
    d_fc_bias = jnp.sum(grad_pre, axis=(0, 1))
    grad_norm = jnp.einsum("bsf,wf->bsw", grad_pre_low, fc_weight, preferred_element_type=jnp.float32)
    grad_ln, d_ln2_gain, d_ln2_bias = layer_norm_bwd(grad_norm, hat_two, inv_two, ln2_gain)
    grad_middle = grad_wide + grad_ln
    grad_middle_low = grad_middle.astype(jnp.bfloat16)
    d_out_weight = jnp.einsum("bsw,bsv->wv", pad_rows(mixed), grad_middle_low, preferred_element_type=jnp.float32)
    d_out_weight, grad_middle_low = lax.optimization_barrier((d_out_weight, grad_middle_low))
    d_out_bias = jnp.sum(grad_middle, axis=(0, 1))
    grad_mixed = jnp.einsum("bsv,wv->bsw", grad_middle_low, out_weight, preferred_element_type=jnp.float32)
    grad_qkv_low, bias_parts = attention_bwd(qkv_vals, grad_mixed.astype(jnp.bfloat16))
    d_qkv_weight = jnp.einsum("bsw,bsk->wk", pad_rows(normed_one), grad_qkv_low, preferred_element_type=jnp.float32)
    d_qkv_bias = jnp.sum(bias_parts, axis=(0, 1))
    grad_norm = jnp.einsum("bsk,wk->bsw", grad_qkv_low, qkv_weight, preferred_element_type=jnp.float32)
    grad_ln, d_ln1_gain, d_ln1_bias = layer_norm_bwd(grad_norm, hat_one, inv_one, ln1_gain)
    grad_in = (grad_middle + grad_ln).astype(jnp.bfloat16)
    return grad_in, (d_ln1_gain, d_ln1_bias, d_qkv_weight, d_qkv_bias, d_out_weight, d_out_bias,
                     d_ln2_gain, d_ln2_bias, d_fc_weight, d_fc_bias, d_proj_weight, d_proj_bias)


def solution(mesh):
    specs = (P("fsdp"),) * 14

    def gather(shard):
        return lax.all_gather(shard, "fsdp", axis=0, tiled=True)

    def pad_shard(shard):
        return jnp.pad(shard, ((0, ROWS_PAD - ROWS), (0, 0)))

    def unpad(padded):
        columns = padded.shape[1]
        return padded.reshape(DEVICES, ROWS_PAD, columns)[:, :ROWS].reshape(DEVICES * ROWS, columns)

    def device_step(resid_in, grad_out, *shards):
        low = [shard.astype(jnp.bfloat16) for shard in shards]
        (_, _, qkv_weight, _, out_weight, _,
         _, _, fc_weight, _, proj_weight, _) = low
        small = jnp.concatenate([jnp.pad(shards[index][None], ((0, 0), (0, LANES - size)))
                                 for index, size in zip(SMALL_AT, SMALL)], axis=0).astype(jnp.bfloat16)
        both = jnp.concatenate([pad_shard(qkv_weight), pad_shard(out_weight),
                                jnp.pad(small, ((0, ROWS_PAD - len(SMALL)), (0, 0)))], axis=1)
        both_full = gather(both)
        fc_shard, proj_shard = pad_shard(fc_weight), proj_weight
        fc_full = unpad(gather(fc_shard))
        proj_full = gather(proj_shard)
        small_full = both_full[:, -LANES:].reshape(DEVICES, ROWS_PAD, LANES)
        pieces = [small_full[:, row, :size].reshape(DEVICES * size) for row, size in enumerate(SMALL)]
        g1, b1, bqkv, bout, g2, b2, bfc, bproj = pieces
        qkv_full = unpad(both_full[:, :QKV])
        out_full = unpad(both_full[:, QKV:-LANES])
        full = (g1, b1, qkv_full, bqkv, out_full, bout, g2, b2, fc_full, bfc, proj_full, bproj)
        resid_out, saved = forward_local(full, resid_in)
        weights = (g1, qkv_full, out_full, g2, fc_full, proj_full)
        grad_in, grads = backward_local(weights, saved, grad_out)
        (d_g1, d_b1, d_qkv, d_bqkv, d_out, d_bout, d_g2, d_b2, d_fc, d_bfc, d_proj, d_bproj) = grads

        def scatter(grad):
            return lax.psum_scatter(grad, "fsdp", scatter_dimension=0, tiled=True)

        proj_part = scatter(d_proj)
        fc_part = scatter(d_fc)[:ROWS]
        out_part = scatter(d_out)[:ROWS]
        qkv_part = scatter(d_qkv)[:ROWS]
        packed = jnp.concatenate([jnp.pad(grad.reshape(DEVICES, 1, size), ((0, 0), (0, 0), (0, LANES - size)))
                                  for grad, size in zip((d_g1, d_b1, d_bqkv, d_bout, d_g2, d_b2, d_bfc, d_bproj), SMALL)], axis=1)
        small_sums = jnp.sum(lax.all_to_all(packed, "fsdp", split_axis=0, concat_axis=0, tiled=True), axis=0)
        small_parts = [small_sums[row, :size] for row, size in enumerate(SMALL)]
        s_g1, s_b1, s_bqkv, s_bout, s_g2, s_b2, s_bfc, s_bproj = small_parts
        return (resid_out, grad_in, s_g1, s_b1, qkv_part, s_bqkv, out_part, s_bout,
                s_g2, s_b2, fc_part, s_bfc, proj_part, s_bproj)

    return jax.shard_map(device_step, mesh=mesh, in_specs=specs, out_specs=specs, check_vma=False)
```

```python
import math
import jax
import jax.numpy as jnp
from jax import lax
from jax.experimental import pallas as pl
from jax.experimental.pallas import tpu as pltpu
from jax.sharding import PartitionSpec as P


HEADS = 16
LN_EPS = 1e-5
DEVICES = 32
ROWS = 44
ROWS_PAD = 48
HALF = DEVICES // 2 * ROWS_PAD
QKV = 4224
LANES = 256
SMALL_AT = (0, 1, 3, 5, 6, 7, 9, 11)
SMALL = (44, 44, 132, 44, 44, 44, 192, 44)


HEAD_DIM = 88
WIDTH = 1408


def dot_nn(left, right):
    return lax.dot_general(left, right, (((1,), (0,)), ((), ())), preferred_element_type=jnp.float32)


def dot_nt(left, right):
    return lax.dot_general(left, right, (((1,), (1,)), ((), ())), preferred_element_type=jnp.float32)


def transposed_probs(query, key):
    scores = dot_nt(key, query) * (HEAD_DIM ** -0.5)
    weights = jnp.exp(scores - jnp.max(scores, axis=0, keepdims=True))
    return weights * (1.0 / jnp.sum(weights, axis=0, keepdims=True))


def attention_fwd_kernel(qkv_ref, mixed_ref):
    for head in range(HEADS):
        query, key, value = (qkv_ref[0, :, pl.ds(part * WIDTH + head * HEAD_DIM, HEAD_DIM)] for part in range(3))
        probs = transposed_probs(query, key).astype(jnp.bfloat16)
        mixed = dot_nn(value.T, probs)
        mixed_ref[0, :, pl.ds(head * HEAD_DIM, HEAD_DIM)] = mixed.T.astype(jnp.bfloat16)


def attention_bwd_kernel(qkv_ref, grad_mixed_ref, grad_qkv_ref, bias_ref):
    for head in range(HEADS):
        query, key, value = (qkv_ref[0, :, pl.ds(part * WIDTH + head * HEAD_DIM, HEAD_DIM)] for part in range(3))
        grad_mixed = grad_mixed_ref[0, :, pl.ds(head * HEAD_DIM, HEAD_DIM)]
        probs = transposed_probs(query, key)
        grad_probs = dot_nt(value, grad_mixed)
        grad_value = dot_nn(probs.astype(jnp.bfloat16), grad_mixed)
        inner = jnp.sum(grad_probs * probs, axis=0, keepdims=True)
        grad_scores = (probs * (grad_probs - inner) * (HEAD_DIM ** -0.5)).astype(jnp.bfloat16)
        grad_key = dot_nn(grad_scores, query)
        grad_query = dot_nn(key.T, grad_scores).T
        for part, grad in enumerate((grad_query, grad_key, grad_value)):
            lanes = pl.ds(part * WIDTH + head * HEAD_DIM, HEAD_DIM)
            grad_qkv_ref[0, :, lanes] = grad.astype(jnp.bfloat16)
            bias_ref[0, :, lanes] = jnp.sum(grad, axis=0, keepdims=True)


def image_block(rows, columns):
    return pl.BlockSpec((1, rows, columns), lambda image: (image, 0, 0))


def attention_fwd(qkv):
    images, tokens, _ = qkv.shape
    return pl.pallas_call(
        attention_fwd_kernel, grid=(images,), name="attention_fwd",
        in_specs=[image_block(tokens, 3 * WIDTH)], out_specs=image_block(tokens, WIDTH),
        out_shape=jax.ShapeDtypeStruct((images, tokens, WIDTH), jnp.bfloat16),
        compiler_params=pltpu.CompilerParams(vmem_limit_bytes=40 << 20),
        cost_estimate=pl.CostEstimate(flops=6_000_000_000, bytes_accessed=9_000_000, transcendentals=3_200_000),
    )(qkv)


def attention_bwd(qkv, grad_mixed):
    images, tokens, _ = qkv.shape
    return pl.pallas_call(
        attention_bwd_kernel, grid=(images,), name="attention_bwd",
        in_specs=[image_block(tokens, 3 * WIDTH), image_block(tokens, WIDTH)],
        out_specs=[image_block(tokens, 3 * WIDTH), image_block(1, 3 * WIDTH)],
        out_shape=[jax.ShapeDtypeStruct((images, tokens, 3 * WIDTH), jnp.bfloat16),
                   jax.ShapeDtypeStruct((images, 1, 3 * WIDTH), jnp.float32)],
        compiler_params=pltpu.CompilerParams(vmem_limit_bytes=40 << 20),
        cost_estimate=pl.CostEstimate(flops=16_000_000_000, bytes_accessed=16_000_000, transcendentals=3_200_000),
    )(qkv, grad_mixed)


def layer_norm_fwd(values, gain, bias):
    mean_val = jnp.mean(values, axis=-1, keepdims=True)
    centered = values - mean_val
    inv_std = lax.rsqrt(jnp.mean(centered * centered, axis=-1, keepdims=True) + LN_EPS)
    x_hat = centered * inv_std
    return x_hat * gain + bias, x_hat, inv_std


def layer_norm_bwd(grad_norm, x_hat, inv_std, gain):
    grad_hat = grad_norm * gain
    grad_vals = inv_std * (grad_hat - jnp.mean(grad_hat, axis=-1, keepdims=True)
                           - x_hat * jnp.mean(grad_hat * x_hat, axis=-1, keepdims=True))
    return grad_vals, jnp.sum(grad_norm * x_hat, axis=(0, 1)), jnp.sum(grad_norm, axis=(0, 1))


def forward_local(full, tokens):
    (ln1_gain, ln1_bias, qkv_weight, qkv_bias, out_weight, out_bias,
     ln2_gain, ln2_bias, fc_weight, fc_bias, proj_weight, proj_bias) = full
    resid = tokens.astype(jnp.float32)
    normed, hat_one, inv_one = layer_norm_fwd(resid, ln1_gain, ln1_bias)
    normed_one = normed.astype(jnp.bfloat16)
    qkv_vals = (jnp.einsum("bsw,wk->bsk", normed_one, qkv_weight, preferred_element_type=jnp.float32) + qkv_bias).astype(jnp.bfloat16)
    mixed = attention_fwd(qkv_vals)
    middle = (resid + jnp.einsum("bsw,wv->bsv", mixed, out_weight, preferred_element_type=jnp.float32) + out_bias).astype(jnp.bfloat16)
    middle_wide = middle.astype(jnp.float32)
    normed, hat_two, inv_two = layer_norm_fwd(middle_wide, ln2_gain, ln2_bias)
    normed_two = normed.astype(jnp.bfloat16)
    pre_act = jnp.einsum("bsw,wf->bsf", normed_two, fc_weight, preferred_element_type=jnp.float32) + fc_bias
    hidden = jax.nn.gelu(pre_act, approximate=False).astype(jnp.bfloat16)
    resid_out = (middle_wide + jnp.einsum("bsf,fw->bsw", hidden, proj_weight, preferred_element_type=jnp.float32) + proj_bias).astype(jnp.bfloat16)
    saved = (hat_one, inv_one, normed_one, qkv_vals, mixed, hat_two, inv_two, normed_two, pre_act, hidden)
    return resid_out, saved


def core_of_chip():
    return lax.axis_index("fsdp") % 2


def swap(values):
    return lax.ppermute(values, "fsdp", [(device, device ^ 1) for device in range(DEVICES)])


def split_columns(values, block, block_pad):
    width = values.shape[-1]
    source = lax.broadcasted_iota(jnp.int32, (width, 2 * HALF), 0)
    target = lax.broadcasted_iota(jnp.int32, (width, 2 * HALF), 1)
    chunk = source // block
    place = chunk // 2 * block_pad + source % block + jnp.where(chunk % 2 == core_of_chip(), 0, HALF)
    spread = (place == target).astype(jnp.bfloat16)
    both = jnp.einsum("bsw,wp->bsp", values, spread, preferred_element_type=jnp.float32).astype(jnp.bfloat16)
    return both[..., :HALF], both[..., HALF:]


def chip_product(left, left_other, right, right_other):
    own = jnp.einsum("bsm,bsn->mn", left, right, preferred_element_type=jnp.float32)
    return own + jnp.einsum("bsm,bsn->mn", left_other, right_other, preferred_element_type=jnp.float32)


def rows_gradient(inputs, grads):
    mine, theirs = split_columns(inputs, ROWS, ROWS_PAD)
    return chip_product(mine, swap(theirs), grads, swap(grads))


def columns_gradient(inputs, grads):
    mine, theirs = split_columns(grads, WIDTH // 2, HALF)
    return chip_product(inputs, swap(inputs), mine, swap(theirs))


def backward_local(weights, saved, grad_out):
    (ln1_gain, qkv_weight, out_weight, ln2_gain, fc_weight, proj_weight) = weights
    (hat_one, inv_one, normed_one, qkv_vals, mixed, hat_two, inv_two, normed_two, pre_act, hidden) = saved
    grad_wide = grad_out.astype(jnp.float32)
    d_proj_weight = columns_gradient(hidden, grad_out)
    d_proj_weight, grad_out = lax.optimization_barrier((d_proj_weight, grad_out))
    d_proj_bias = jnp.sum(grad_wide, axis=(0, 1))
    grad_hidden = jnp.einsum("bsw,fw->bsf", grad_out, proj_weight, preferred_element_type=jnp.float32)
    gauss_cdf = 0.5 * (1.0 + lax.erf(pre_act * (0.5 ** 0.5)))
    gauss_pdf = jnp.exp(-0.5 * pre_act * pre_act) * ((2.0 * math.pi) ** -0.5)
    grad_pre = grad_hidden * (gauss_cdf + pre_act * gauss_pdf)
    grad_pre_low = grad_pre.astype(jnp.bfloat16)
    d_fc_weight = rows_gradient(normed_two, grad_pre_low)
    d_fc_weight, grad_pre_low = lax.optimization_barrier((d_fc_weight, grad_pre_low))
    d_fc_bias = jnp.sum(grad_pre, axis=(0, 1))
    grad_norm = jnp.einsum("bsf,wf->bsw", grad_pre_low, fc_weight, preferred_element_type=jnp.float32)
    grad_ln, d_ln2_gain, d_ln2_bias = layer_norm_bwd(grad_norm, hat_two, inv_two, ln2_gain)
    grad_middle = grad_wide + grad_ln
    grad_middle_low = grad_middle.astype(jnp.bfloat16)
    d_out_weight = rows_gradient(mixed, grad_middle_low)
    d_out_weight, grad_middle_low = lax.optimization_barrier((d_out_weight, grad_middle_low))
    d_out_bias = jnp.sum(grad_middle, axis=(0, 1))
    grad_mixed = jnp.einsum("bsv,wv->bsw", grad_middle_low, out_weight, preferred_element_type=jnp.float32)
    grad_qkv_low, bias_parts = attention_bwd(qkv_vals, grad_mixed.astype(jnp.bfloat16))
    d_qkv_weight = rows_gradient(normed_one, grad_qkv_low)
    d_qkv_bias = jnp.sum(bias_parts, axis=(0, 1))
    grad_norm = jnp.einsum("bsk,wk->bsw", grad_qkv_low, qkv_weight, preferred_element_type=jnp.float32)
    grad_ln, d_ln1_gain, d_ln1_bias = layer_norm_bwd(grad_norm, hat_one, inv_one, ln1_gain)
    grad_in = (grad_middle + grad_ln).astype(jnp.bfloat16)
    return grad_in, (d_ln1_gain, d_ln1_bias, d_qkv_weight, d_qkv_bias, d_out_weight, d_out_bias,
                     d_ln2_gain, d_ln2_bias, d_fc_weight, d_fc_bias, d_proj_weight, d_proj_bias)


def solution(mesh):
    specs = (P("fsdp"),) * 14

    def gather(shard):
        return lax.all_gather(shard, "fsdp", axis=0, tiled=True)

    def pad_shard(shard):
        return jnp.pad(shard, ((0, ROWS_PAD - ROWS), (0, 0)))

    def unpad(padded):
        columns = padded.shape[1]
        return padded.reshape(DEVICES, ROWS_PAD, columns)[:, :ROWS].reshape(DEVICES * ROWS, columns)

    def device_step(resid_in, grad_out, *shards):
        low = [shard.astype(jnp.bfloat16) for shard in shards]
        (_, _, qkv_weight, _, out_weight, _,
         _, _, fc_weight, _, proj_weight, _) = low
        small = jnp.concatenate([jnp.pad(shards[index][None], ((0, 0), (0, LANES - size)))
                                 for index, size in zip(SMALL_AT, SMALL)], axis=0).astype(jnp.bfloat16)
        both = jnp.concatenate([pad_shard(qkv_weight), pad_shard(out_weight),
                                jnp.pad(small, ((0, ROWS_PAD - len(SMALL)), (0, 0)))], axis=1)
        both_full = gather(both)
        fc_shard, proj_shard = pad_shard(fc_weight), proj_weight
        fc_full = unpad(gather(fc_shard))
        proj_full = gather(proj_shard)
        small_full = both_full[:, -LANES:].reshape(DEVICES, ROWS_PAD, LANES)
        pieces = [small_full[:, row, :size].reshape(DEVICES * size) for row, size in enumerate(SMALL)]
        g1, b1, bqkv, bout, g2, b2, bfc, bproj = pieces
        qkv_full = unpad(both_full[:, :QKV])
        out_full = unpad(both_full[:, QKV:-LANES])
        full = (g1, b1, qkv_full, bqkv, out_full, bout, g2, b2, fc_full, bfc, proj_full, bproj)
        resid_out, saved = forward_local(full, resid_in)
        weights = (g1, qkv_full, out_full, g2, fc_full, proj_full)
        grad_in, grads = backward_local(weights, saved, grad_out)
        (d_g1, d_b1, d_qkv, d_bqkv, d_out, d_bout, d_g2, d_b2, d_fc, d_bfc, d_proj, d_bproj) = grads

        def scatter(grad):
            groups = [list(range(core, DEVICES, 2)) for core in range(2)]
            return lax.psum_scatter(grad, "fsdp", scatter_dimension=0, tiled=True, axis_index_groups=groups)

        proj_part = scatter(d_proj)
        core, proj_rows = core_of_chip(), proj_part.shape[0] // 2
        mine = lax.dynamic_slice_in_dim(proj_part, core * proj_rows, proj_rows)
        theirs = swap(lax.dynamic_slice_in_dim(proj_part, (1 - core) * proj_rows, proj_rows))
        proj_part = jnp.concatenate([jnp.where(core == 0, mine, theirs)[:, :WIDTH // 2],
                                     jnp.where(core == 0, theirs, mine)[:, :WIDTH // 2]], axis=1)
        fc_part = scatter(d_fc)[:ROWS]
        out_part = scatter(d_out)[:ROWS]
        qkv_part = scatter(d_qkv)[:ROWS]
        packed = jnp.concatenate([jnp.pad(grad.reshape(DEVICES, 1, size), ((0, 0), (0, 0), (0, LANES - size)))
                                  for grad, size in zip((d_g1, d_b1, d_bqkv, d_bout, d_g2, d_b2, d_bfc, d_bproj), SMALL)], axis=1)
        small_sums = jnp.sum(lax.all_to_all(packed, "fsdp", split_axis=0, concat_axis=0, tiled=True), axis=0)
        small_parts = [small_sums[row, :size] for row, size in enumerate(SMALL)]
        s_g1, s_b1, s_bqkv, s_bout, s_g2, s_b2, s_bfc, s_bproj = small_parts
        return (resid_out, grad_in, s_g1, s_b1, qkv_part, s_bqkv, out_part, s_bout,
                s_g2, s_b2, fc_part, s_bfc, proj_part, s_bproj)

    return jax.shard_map(device_step, mesh=mesh, in_specs=specs, out_specs=specs, check_vma=False)
```
